32 devices in a mesh: dp: 4 (over y, core), tp: 8 (over z, x).
Axes of the slice: x: 2, y: 2, z: 4, core: 2. Of those that a mesh axis runs over, the one named last changes fastest.
Arguments:
- tokens: bfloat16 [1024, 7168], P(('dp', 'tp')), may hold values from -6 to 6
- w_gate: bfloat16 [7168, 12288], P(None, 'tp'), may hold values from -0.0625 to 0.0625
- w_up: bfloat16 [7168, 12288], P(None, 'tp'), may hold values from -0.0625 to 0.0625
- w_down: bfloat16 [12288, 7168], P('tp'), may hold values from -0.0546875 to 0.0546875
- cotangent: bfloat16 [1024, 7168], P(('dp', 'tp')), may hold values from -6 to 6
Outputs:
- mixed: bfloat16 [1024, 7168], P(('dp', 'tp'))
- input_grad: bfloat16 [1024, 7168], P(('dp', 'tp'))
- gate_grad: float32 [7168, 12288], P('dp', 'tp')
- up_grad: float32 [7168, 12288], P('dp', 'tp')
- down_grad: float32 [12288, 7168], P('tp', 'dp')
The draws below stay inside these ranges and needn't reach their ends.
All inputs are finite; a program needn't handle non-finite values.
Results may differ from the reference program's by a relative error of at most 0.0049.
Values may be sent and summed in bfloat16 or wider, within the bound.
A program may use at most 192 MiB of HBM per device.

```python
import jax
import jax.numpy as jnp

D = 7168
FF = 12288
TOKENS = 1024


def shard_levels(key, shape, cuts, low, largest):
    def one(dim, parts):
        steps = jax.random.uniform(jax.random.fold_in(jax.random.fold_in(key, 6), dim), (parts,), jnp.float32, low / len(cuts), largest / len(cuts))
        return jnp.repeat(jnp.exp(steps), shape[dim] // parts).reshape((-1,) + (1,) * (len(shape) - dim - 1))

    loudness = one(*cuts[0])
    for cut in cuts[1:]:
        loudness = loudness * one(*cut)
    return loudness


def gaussian(own_key, extent, scale, reach, cuts=(), held_as=jnp.bfloat16):
    loudness = shard_levels(own_key, extent, cuts, -0.22, 0.18) if cuts else 1.0
    drawn = jax.random.normal(own_key, extent, jnp.float32) * scale * loudness
    return jnp.minimum(jnp.maximum(drawn, -reach), reach).astype(held_as)


def setup_inputs(seed: int = 0) -> dict:
    arg_keys = jax.random.split(jax.random.key(seed), 6)
    return {
        "tokens": gaussian(arg_keys[0], (TOKENS, D), 1.0, 6.0, ((0, 32),)),
        "w_gate": gaussian(arg_keys[1], (D, FF), D ** -0.5, 0.0625, ((1, 8),)),
        "w_up": gaussian(arg_keys[2], (D, FF), D ** -0.5, 0.0625, ((1, 8),)),
        "w_down": gaussian(arg_keys[3], (FF, D), FF ** -0.5, 0.0546875, ((0, 8),)),
        "cotangent": gaussian(arg_keys[4], (TOKENS, D), 1.0, 6.0, ((0, 32),)),
    }


def reference(tokens, w_gate, w_up, w_down, cotangent):
    gate = jnp.dot(tokens, w_gate, preferred_element_type=jnp.float32)
    up = jnp.dot(tokens, w_up, preferred_element_type=jnp.float32)
    sig = jax.nn.sigmoid(gate)
    act = gate * sig
    hidden = (act * up).astype(jnp.bfloat16)
    mixed = jnp.dot(hidden, w_down, preferred_element_type=jnp.float32).astype(jnp.bfloat16)
    back = jnp.dot(cotangent, w_down.T, preferred_element_type=jnp.float32)
    dgate = (back * up * sig * (1.0 + gate * (1.0 - sig))).astype(jnp.bfloat16)
    dup = (back * act).astype(jnp.bfloat16)
    input_grad = (jnp.dot(dgate, w_gate.T, preferred_element_type=jnp.float32)
                  + jnp.dot(dup, w_up.T, preferred_element_type=jnp.float32)).astype(jnp.bfloat16)
    gate_grad = jnp.dot(tokens.T, dgate, preferred_element_type=jnp.float32)
    up_grad = jnp.dot(tokens.T, dup, preferred_element_type=jnp.float32)
    down_grad = jnp.dot(hidden.T, cotangent, preferred_element_type=jnp.float32)
    return mixed, input_grad, gate_grad, up_grad, down_grad
```

```python
import functools

import jax
import jax.numpy as jnp
from jax import lax
from jax.experimental import pallas as pl
from jax.experimental.pallas import tpu as pltpu
from jax.sharding import PartitionSpec as P


BF16 = jnp.bfloat16
F32 = jnp.float32


def right_trans(left, matrix):
    return lax.dot_general(left, matrix, (((1,), (1,)), ((), ())), preferred_element_type=F32)


def send_xor(block, bit, count):
    return lax.ppermute(block, "dp", [(i, i ^ bit) for i in range(count)])


def send_tp(block, dz, dx, count):
    ring = count // 2
    perm = [(i, ((i // 2 + dz) % ring) * 2 + ((i % 2) ^ dx)) for i in range(count)]
    return lax.ppermute(block, "tp", perm)


def gather_tp(own, count):
    if count != 8:
        whole = lax.all_gather(own, "tp", axis=0)
        return [whole[i] for i in range(count)]
    send = functools.partial(send_tp, count=count)
    across = send(own, 0, 1)
    below = send(own, 1, 0)
    above = send(own, -1, 0)
    across_above = send(above, 0, 1)
    across_below = send(across, 1, 0)
    far = send(above, -1, 0)
    half = own.shape[1] // 256 * 128
    left, right = across_above[:, :half], across_below[:, half:]
    left, right = send(left, -1, 0), send(right, 1, 0)
    across_far = jnp.concatenate([left, right], axis=1)
    return [own, across, above, across_above, far, across_far, below, across_below]


def scatter_tp(partial, count):
    rows = partial.shape[0] // count
    if count != 8:
        return lax.psum_scatter(partial.astype(F32), "tp", scatter_dimension=0, tiled=True).astype(BF16)
    send = functools.partial(send_tp, count=count)
    half = partial.shape[1] // 256 * 128
    near, above, far, below = (partial[i * 2 * rows : (i + 1) * 2 * rows] for i in range(4))
    left, right = far[:, :half], far[:, half:]
    from_below, from_above = send(left, 1, 0), send(right, -1, 0)
    up = jnp.concatenate(
        [(above[:, :half].astype(F32) + from_below.astype(F32)).astype(BF16), above[:, half:]], axis=1
    )
    down = jnp.concatenate(
        [below[:, :half], (below[:, half:].astype(F32) + from_above.astype(F32)).astype(BF16)], axis=1
    )
    up, down = send(up, 1, 0), send(down, -1, 0)
    total = near.astype(F32) + up.astype(F32) + down.astype(F32)
    crossed = total[rows:].astype(BF16)
    crossed = send(crossed, 0, 1)
    return (total[:rows] + crossed.astype(F32)).astype(BF16)


def gather_dp(own, count):
    blocks = {0: own}
    bit = count // 2
    while bit:
        blocks.update({k | bit: send_xor(b, bit, count) for k, b in list(blocks.items())})
        bit //= 2
    return [blocks[k] for k in range(count)]


def grad_kernel(count, *refs):
    lefts, rights, out = refs[:count], refs[count : 2 * count], refs[-1]
    total = None
    for left, right in zip(lefts, rights):
        part = lax.dot_general(
            left[...], right[...], (((0,), (0,)), ((), ())), preferred_element_type=F32
        )
        total = part if total is None else total + part
    out[...] = total


def token_sum(lefts, rights):
    count = len(lefts)
    tokens, rows = lefts[0].shape
    cols = rights[0].shape[1]
    tile = 256 if rows % 256 == 0 else 128
    return pl.pallas_call(
        functools.partial(grad_kernel, count),
        grid=(rows // tile,),
        in_specs=[pl.BlockSpec((tokens, tile), lambda i: (0, i))] * count
        + [pl.BlockSpec((tokens, cols), lambda i: (0, 0))] * count,
        out_specs=pl.BlockSpec((tile, cols), lambda i: (i, 0)),
        out_shape=jax.ShapeDtypeStruct((rows, cols), F32),
        cost_estimate=pl.CostEstimate(
            flops=2 * count * tokens * rows * cols,
            bytes_accessed=2 * count * tokens * (rows + cols) + 4 * rows * cols,
            transcendentals=0,
        ),
        compiler_params=pltpu.CompilerParams(vmem_limit_bytes=32 << 20),
    )(*lefts, *rights)


def body(dp, tp, tokens, w_gate, w_up, w_down, cotangent):
    me = lax.axis_index("dp")
    part = tokens.shape[1] // dp

    def features(x, k):
        return lax.dynamic_slice_in_dim(x, (me ^ k) * part, part, axis=1)

    gathered = jnp.concatenate(gather_tp(tokens, tp), axis=0)
    gate = jnp.dot(gathered, w_gate, preferred_element_type=F32)
    up = jnp.dot(gathered, w_up, preferred_element_type=F32)

    grads = gather_tp(cotangent, tp)
    grad_full = jnp.concatenate(grads, axis=0)

    sig = jax.nn.sigmoid(gate)
    act = gate * sig
    hidden = (act * up).astype(BF16)
    gate, up, hidden = lax.optimization_barrier((gate, up, hidden))
    mixed = jnp.dot(hidden, w_down, preferred_element_type=F32).astype(BF16)
    sig = jax.nn.sigmoid(gate)
    act = gate * sig
    back = right_trans(grad_full, w_down)
    dgate = (back * up * sig * (1.0 + gate * (1.0 - sig))).astype(BF16)
    dup = (back * act).astype(BF16)

    mixed = scatter_tp(mixed, tp)
    partial = (right_trans(dgate, w_gate) + right_trans(dup, w_up)).astype(BF16)
    input_grad = scatter_tp(partial, tp)

    token_parts = [features(gathered, 0)] + [
        send_xor(features(gathered, k), k, dp) for k in range(1, dp)
    ]

    far = [send_xor(features(cotangent, k), k, dp) for k in range(2, dp)]
    rows = cotangent.shape[0]
    far = gather_tp(jnp.concatenate(far, axis=0), tp)
    grad_parts = [features(grad_full, 0), send_xor(features(grad_full, 1), 1, dp)] + [
        jnp.concatenate([f[i * rows : (i + 1) * rows] for f in far], axis=0) for i in range(dp - 2)
    ]

    all_hidden = gather_dp(hidden, dp)
    all_dgate = gather_dp(dgate, dp)
    all_dup = gather_dp(dup, dp)
    down_grad = token_sum(all_hidden, grad_parts)
    gate_grad = token_sum(token_parts, all_dgate)
    up_grad = token_sum(token_parts, all_dup)
    return (mixed, input_grad, gate_grad, up_grad, down_grad)


MESH = pl.DeviceIdType.MESH
CORES, COLS = 2, 2


def fused_kernel(
    tokens, cotangent, w_gate, w_up, w_down,
    mixed, input_grad, features, units,
    blocks, gate, up, back, hidden, dgate, dup, partial, from_x, from_below, from_above, onward,
    gu_tiles, down_tiles, in_tiles,
    own_sem, gu_sem, down_sem, in_sem,
    up_send, up_recv, dn_send, dn_recv, x_send, x_recv,
    ex_send, ex_recv, un_send, un_recv, un_local,
    rx_send, rx_recv, rz_send, ru_recv, rd_recv,
):
    me, place = lax.axis_index("dp"), lax.axis_index("tp")
    z, x = place // COLS, place % COLS
    y, core = me // CORES, me % CORES
    rows, _ = tokens.shape
    steps, held, part = blocks.shape[0] // 2, blocks.shape[1], blocks.shape[2]
    levels = held // rows // COLS
    column = levels * rows
    inner = gate.shape[1]
    half, slab = inner // 2, part // 2
    top = levels - 1
    beside = (me, z * COLS + (1 - x))
    above, below = (me, place + COLS), (me, place - COLS)
    twin = y * CORES + (1 - core)
    across = (1 - y) * CORES + core

    def chunk(g):
        s = lax.rem(g, steps)
        return lax.rem(s + 1 + y, 2) * 2 + s // 2

    def remote(src, dst, send, recv, device):
        return pltpu.make_async_remote_copy(
            src_ref=src, dst_ref=dst, send_sem=send, recv_sem=recv, device_id=device, device_id_type=MESH
        )

    def spot(g, col, level):
        return blocks.at[g, pl.ds(pl.multiple_of((col * levels + level) * rows, rows), rows), :]

    def go_up(g, h):
        ref = spot(g, x, z - h)
        return remote(ref, ref, up_send.at[g, h], up_recv.at[g, h], above)

    def go_down(g, h):
        ref = spot(g, x, z + h)
        return remote(ref, ref, dn_send.at[g, h], dn_recv.at[g, h], below)

    def go_x(g, level):
        ref = spot(g, x, level)
        return remote(ref, ref, x_send.at[g, level], x_recv.at[g, level], beside)

    def own(g):
        @pl.when(z < top)
        def _():
            go_up(g, 0).start()

        @pl.when(z > 0)
        def _():
            go_down(g, 0).start()

        go_x(g, z).start()

    def relay(g, h):
        @pl.when(z >= h)
        def _():
            ref = spot(g, x, z - h)
            remote(ref, ref, up_send.at[g, h - 1], up_recv.at[g, h - 1], below).wait_recv()
            if h < top:
                @pl.when(z < top)
                def _():
                    go_up(g, h).start()

            go_x(g, z - h).start()

        @pl.when(z + h <= top)
        def _():
            ref = spot(g, x, z + h)
            remote(ref, ref, dn_send.at[g, h - 1], dn_recv.at[g, h - 1], above).wait_recv()
            if h < top:
                @pl.when(z > 0)
                def _():
                    go_down(g, h).start()

            go_x(g, z + h).start()

    def arrived(g):
        for level in range(levels):
            ref = spot(g, 1 - x, level)
            remote(ref, ref, x_send.at[g, level], x_recv.at[g, level], beside).wait_recv()

    def exchange(g):
        to, kind = chunk(g), g // steps

        @pl.when(to == me)
        def _():
            pltpu.make_async_copy(blocks.at[g], features.at[kind, me], ex_send.at[g]).start()

        @pl.when(to != me)
        def _():
            remote(
                blocks.at[g], features.at[kind, me], ex_send.at[g], ex_recv.at[kind, me], (to, place)
            ).start()

    def exchange_done(g):
        to, kind = chunk(g), g // steps

        @pl.when(to == me)
        def _():
            pltpu.make_async_copy(blocks.at[g], features.at[kind, me], ex_send.at[g]).wait()

        @pl.when(to != me)
        def _():
            remote(
                blocks.at[g], features.at[kind, me], ex_send.at[g], ex_recv.at[kind, me], (to, place)
            ).wait_send()

    def units_copies(src, k):
        dst = units.at[k, me]
        return (
            pltpu.make_async_copy(src, dst, un_local.at[k]),
            remote(src, dst, un_send.at[k, 0], un_recv.at[k, me], (across, place)),
            remote(src, dst, un_send.at[k, 1], un_recv.at[k, me], (twin, place)),
        )

    def units_forward(k):
        ref = units.at[k, across]
        return remote(ref, ref, un_send.at[k, 2], un_recv.at[k, across], (twin, place))

    def units_arrived(k, who):
        ref = units.at[k, who]
        remote(ref, ref, un_send.at[k, 2], un_recv.at[k, who], (twin, place)).wait_recv()

    def gu_copy(g, t):
        source = w_gate if t < 2 else w_up
        return pltpu.make_async_copy(
            source.at[pl.ds(pl.multiple_of(chunk(g) * part, 128), part), (t % 2) * half : (t % 2 + 1) * half],
            gu_tiles.at[t % 2],
            gu_sem.at[t % 2],
        )

    def down_copy(g, t):
        return pltpu.make_async_copy(
            w_down.at[t * half : (t + 1) * half, pl.ds(pl.multiple_of(chunk(g) * part, 128), part)],
            down_tiles.at[t],
            down_sem.at[t],
        )

    def in_copy(j, t, k):
        start = chunk(j) * part + t * slab
        return pltpu.make_async_copy(
            (w_gate, w_up)[k].at[pl.ds(pl.multiple_of(start, 128), slab), :],
            in_tiles.at[t, k],
            in_sem.at[t, k],
        )

    def rs_x(q):
        src = partial.at[q, pl.ds(pl.multiple_of((1 - x) * column, rows), column), :]
        return remote(src, from_x.at[q], rx_send.at[q], rx_recv.at[q], beside)

    def rs_up(q, first, count):
        return remote(
            onward.at[q, first * rows : (first + count) * rows, :],
            from_below.at[q, 0 : count * rows, :],
            rz_send.at[q, 0], ru_recv.at[q], above,
        )

    def rs_down(q, first, count):
        return remote(
            onward.at[q, first * rows : (first + count) * rows, :],
            from_above.at[q, 0 : count * rows, :],
            rz_send.at[q, 1], rd_recv.at[q], below,
        )

    def below_arrived(q, count):
        ref = from_below.at[q, 0 : count * rows, :]
        remote(ref, ref, rz_send.at[q, 0], ru_recv.at[q], below).wait_recv()

    def above_arrived(q, count):
        ref = from_above.at[q, 0 : count * rows, :]
        remote(ref, ref, rz_send.at[q, 1], rd_recv.at[q], above).wait_recv()

    def total(q, level, *more):
        mine = partial[q, pl.ds(pl.multiple_of(x * column + level * rows, rows), rows), :].astype(F32)
        mine += from_x[q, level * rows : (level + 1) * rows, :].astype(F32)
        for ref, at in more:
            mine += ref[q, at * rows : (at + 1) * rows, :].astype(F32)
        return mine.astype(BF16)

    def put(q, at, value):
        onward[q, at * rows : (at + 1) * rows, :] = value

    def emit(q, value):
        cols = pl.ds(pl.multiple_of(chunk(q) * part, 128), part)

        @pl.when(q < steps)
        def _():
            mixed[:, cols] = value

        @pl.when(q >= steps)
        def _():
            input_grad[:, cols] = value

    def stage_one(q):
        rs_x(q).wait_recv()

        @pl.when(z == 0)
        def _():
            for level in (1, 2, 3):
                put(q, level - 1, total(q, level))
            rs_up(q, 0, 3).start()

        @pl.when(z == 3)
        def _():
            for level in (0, 1, 2):
                put(q, level, total(q, level))
            rs_down(q, 0, 3).start()

    def stage_two(q):
        @pl.when(z == 1)
        def _():
            below_arrived(q, 3)
            for level in (2, 3):
                put(q, level - 2, total(q, level, (from_below, level - 1)))
            rs_up(q, 0, 2).start()

        @pl.when(z == 2)
        def _():
            above_arrived(q, 3)
            for level in (0, 1):
                put(q, level, total(q, level, (from_above, level)))
            rs_down(q, 0, 2).start()

    def stage_three(q):
        @pl.when(z == 2)
        def _():
            below_arrived(q, 2)
            put(q, 2, total(q, 3, (from_below, 1)))
            rs_up(q, 2, 1).start()

        @pl.when(z == 1)
        def _():
            above_arrived(q, 2)
            put(q, 2, total(q, 0, (from_above, 0)))
            rs_down(q, 2, 1).start()

    def stage_four(q):
        @pl.when(z == 0)
        def _():
            above_arrived(q, 1)
            emit(q, total(q, 0, (from_above, 0)))

        @pl.when(z == 1)
        def _():
            emit(q, total(q, 1, (from_below, 0), (from_above, 1)))

        @pl.when(z == 2)
        def _():
            emit(q, total(q, 2, (from_below, 0), (from_above, 2)))

        @pl.when(z == 3)
        def _():
            below_arrived(q, 1)
            emit(q, total(q, 3, (from_below, 0)))

    mine = pl.ds(pl.multiple_of((x * levels + z) * rows, rows), rows)

    def own_copy(g, source):
        return pltpu.make_async_copy(
            source.at[:, pl.ds(pl.multiple_of(chunk(g) * part, 128), part)], blocks.at[g, mine, :], own_sem.at[g]
        )

    for s in range(steps):
        own_copy(s, tokens).start()
    for s in range(steps):
        own_copy(steps + s, cotangent).start()
    for t in range(2):
        gu_copy(0, t).start()
        down_copy(steps, t).start()
        for k in range(2):
            in_copy(0, t, k).start()

    barrier = pltpu.get_barrier_semaphore()

    def greet(device):
        pl.semaphore_signal(barrier, inc=1, device_id=device, device_id_type=MESH)

    greet(beside)
    for other in (twin, across, (1 - y) * CORES + (1 - core)):
        greet((other, place))

    @pl.when(z < top)
    def _():
        greet(above)

    @pl.when(z > 0)
    def _():
        greet(below)

    @pl.when((z > 0) & (z < top))
    def _():
        pl.semaphore_wait(barrier, 6)

    @pl.when((z == 0) | (z == top))
    def _():
        pl.semaphore_wait(barrier, 5)

    for s in range(steps):
        own_copy(s, tokens).wait()
        own_copy(steps + s, cotangent).wait()

    own(0)
    own(1)
    gate[...] = jnp.zeros_like(gate)
    up[...] = jnp.zeros_like(up)
    back[...] = jnp.zeros_like(back)
    for h in range(1, levels):
        relay(0, h)

    @pl.loop(0, steps)
    def _(g):
        own(g + 2)
        relay(g + 1, 1)
        arrived(g)
        exchange(g)
        for t in range(4):
            gu_copy(g, t).wait()
            target, at = (gate, up)[t // 2], t % 2
            target[:, at * half : (at + 1) * half] += jnp.dot(
                blocks[g], gu_tiles[at], preferred_element_type=F32
            )
            if t < 2:
                gu_copy(g, t + 2).start()
            else:
                @pl.when(g < steps - 1)
                def _():
                    gu_copy(g + 1, t - 2).start()
            if t in (1, 3):
                relay(g + 1, t // 2 + 2)

    lines = 32

    @pl.loop(0, held // lines)
    def _(i):
        at = pl.ds(pl.multiple_of(i * lines, lines), lines)
        value = gate[at, :]
        hidden[at, :] = (value * jax.nn.sigmoid(value) * up[at, :]).astype(BF16)

    for copy in units_copies(hidden, 0):
        copy.start()

    @pl.loop(steps, 2 * steps)
    def _(g):
        @pl.when(g + 2 < 2 * steps)
        def _():
            own(g + 2)

        @pl.when(g + 1 < 2 * steps)
        def _():
            relay(g + 1, 1)

        for t in range(2):
            down_copy(g, t).wait()
        product = jnp.dot(hidden[:, :half], down_tiles[0], preferred_element_type=F32)
        product += jnp.dot(hidden[:, half:], down_tiles[1], preferred_element_type=F32)
        partial[g - steps] = product.astype(BF16)

        @pl.when(g + 1 < 2 * steps)
        def _():
            relay(g + 1, 2)

        arrived(g)
        exchange(g)
        for t in range(2):
            back[:, t * half : (t + 1) * half] += right_trans(blocks[g], down_tiles[t])

            @pl.when(g + 1 < 2 * steps)
            def _():
                down_copy(g + 1, t).start()

        @pl.when(g + 1 < 2 * steps)
        def _():
            relay(g + 1, 3)

        @pl.when(g == 2 * steps - 2)
        def _():
            for j in range(steps - 1):
                rs_x(j).start()

    rs_x(steps - 1).start()

    @pl.loop(0, held // lines)
    def _(i):
        at = pl.ds(pl.multiple_of(i * lines, lines), lines)
        value, other, grad = gate[at, :], up[at, :], back[at, :]
        sig = jax.nn.sigmoid(value)
        dgate[at, :] = (grad * other * sig * (1.0 + value * (1.0 - sig))).astype(BF16)
        dup[at, :] = (grad * (value * sig)).astype(BF16)

    for k, source in ((1, dgate), (2, dup)):
        for copy in units_copies(source, k):
            copy.start()
    units_arrived(0, across)
    units_forward(0).start()

    last = 2 * steps

    @pl.loop(0, last + 3)
    def _(i):
        @pl.when(i < steps)
        def _():
            for t in range(2):
                for k in range(2):
                    in_copy(i, t, k).wait()
                product = right_trans(dgate[...], in_tiles[t, 0]) + right_trans(dup[...], in_tiles[t, 1])
                partial[i + steps, :, t * slab : (t + 1) * slab] = product.astype(BF16)

                @pl.when(i + 1 < steps)
                def _():
                    for k in range(2):
                        in_copy(i + 1, t, k).start()
            rs_x(i + steps).start()

        @pl.when(i < last)
        def _():
            stage_one(i)

        @pl.when((i >= 1) & (i < last + 1))
        def _():
            stage_two(i - 1)

        @pl.when((i >= 2) & (i < last + 2))
        def _():
            stage_three(i - 2)

        @pl.when(i >= 3)
        def _():
            stage_four(i - 3)

        @pl.when(i == last)
        def _():
            units_arrived(1, across)
            units_forward(1).start()

    units_arrived(2, across)
    units_forward(2).start()

    @pl.loop(0, 2 * steps)
    def _(g):
        for h in range(top):
            @pl.when((z < top) & (z >= h))
            def _():
                go_up(g, h).wait_send()

            @pl.when((z > 0) & (z + h <= top))
            def _():
                go_down(g, h).wait_send()

        for level in range(levels):
            go_x(g, level).wait_send()
        exchange_done(g)
        rs_x(g).wait_send()

        @pl.when(z == 0)
        def _():
            rs_up(g, 0, 3).wait_send()

        @pl.when(z == 1)
        def _():
            rs_up(g, 0, 2).wait_send()
            rs_down(g, 2, 1).wait_send()

        @pl.when(z == 2)
        def _():
            rs_up(g, 2, 1).wait_send()
            rs_down(g, 0, 2).wait_send()

        @pl.when(z == 3)
        def _():
            rs_down(g, 0, 3).wait_send()

    for kind in range(2):
        for other in (twin, across, (1 - y) * CORES + (1 - core)):
            ref = features.at[kind, other]
            remote(ref, ref, ex_send.at[0], ex_recv.at[kind, other], (twin, place)).wait_recv()
    for k, source in enumerate((hidden, dgate, dup)):
        local, far, near = units_copies(source, k)
        local.wait()
        far.wait_send()
        near.wait_send()
        units_forward(k).wait_send()
        units_arrived(k, twin)
        units_arrived(k, (1 - y) * CORES + (1 - core))


def fused_body(dp, tp, tokens, w_gate, w_up, w_down, cotangent):
    rows, width = tokens.shape
    inner = w_gate.shape[1]
    held, part = rows * tp, width // dp
    levels = tp // COLS
    half, slab = inner // 2, part // 2
    hbm, vmem = pl.BlockSpec(memory_space=pl.ANY), pl.BlockSpec(memory_space=pltpu.VMEM)
    dma = pltpu.SemaphoreType.DMA
    chain = (levels - 1) * rows
    mixed, input_grad, features, units = pl.pallas_call(
        fused_kernel,
        in_specs=[hbm] * 5,
        out_specs=[vmem, vmem, hbm, hbm],
        out_shape=[
            jax.ShapeDtypeStruct((rows, width), BF16),
            jax.ShapeDtypeStruct((rows, width), BF16),
            jax.ShapeDtypeStruct((2, dp, held, part), BF16),
            jax.ShapeDtypeStruct((3, dp, held, inner), BF16),
        ],
        scratch_shapes=[
            pltpu.VMEM((2 * dp, held, part), BF16),
            pltpu.VMEM((held, inner), F32),
            pltpu.VMEM((held, inner), F32),
            pltpu.VMEM((held, inner), F32),
            pltpu.VMEM((held, inner), BF16),
            pltpu.VMEM((held, inner), BF16),
            pltpu.VMEM((held, inner), BF16),
            pltpu.VMEM((2 * dp, held, part), BF16),
            pltpu.VMEM((2 * dp, levels * rows, part), BF16),
            pltpu.VMEM((2 * dp, chain, part), BF16),
            pltpu.VMEM((2 * dp, chain, part), BF16),
            pltpu.VMEM((2 * dp, chain, part), BF16),
            pltpu.VMEM((2, part, half), BF16),
            pltpu.VMEM((2, half, part), BF16),
            pltpu.VMEM((2, 2, slab, inner), BF16),
            dma((2 * dp,)), dma((2,)), dma((2,)), dma((2, 2)),
            dma((2 * dp, 3)), dma((2 * dp, 3)), dma((2 * dp, 3)), dma((2 * dp, 3)),
            dma((2 * dp, levels)), dma((2 * dp, levels)),
            dma((2 * dp,)), dma((2, dp)),
            dma((3, 3)), dma((3, dp)), dma((3,)),
            dma((2 * dp,)), dma((2 * dp,)), dma((2 * dp, 2)), dma((2 * dp,)), dma((2 * dp,)),
        ],
        compiler_params=pltpu.CompilerParams(
            collective_id=0, has_side_effects=True, vmem_limit_bytes=67_043_328
        ),
        name="fused",
    )(tokens, cotangent, w_gate, w_up, w_down)

    def grad(left, at, right, of):
        count = left.shape[-1]
        cols = right.shape[-1]
        tile = count // 2 if count % 256 == 0 else 128

        def kernel(l_ref, r_ref, out):
            out[...] = lax.dot_general(
                l_ref[...].reshape(dp * held, tile),
                r_ref[...].reshape(dp * held, cols),
                (((0,), (0,)), ((), ())),
                preferred_element_type=F32,
            )

        return pl.pallas_call(
            kernel,
            grid=(count // tile,),
            in_specs=[
                pl.BlockSpec((None, dp, held, tile), lambda i: (at, 0, 0, i)),
                pl.BlockSpec((None, dp, held, cols), lambda i: (of, 0, 0, 0)),
            ],
            out_specs=pl.BlockSpec((tile, cols), lambda i: (i, 0)),
            out_shape=jax.ShapeDtypeStruct((count, cols), F32),
            compiler_params=pltpu.CompilerParams(vmem_limit_bytes=60 << 20),
        )(left, right)

    gate_grad = grad(features, 0, units, 1)
    up_grad = grad(features, 0, units, 2)
    down_grad = grad(units, 0, features, 1)
    return mixed, input_grad, gate_grad, up_grad, down_grad


def solution(mesh):
    in_specs = (
        P(("dp", "tp"), None),
        P(None, "tp"),
        P(None, "tp"),
        P("tp", None),
        P(("dp", "tp"), None),
    )
    out_specs = (
        P(("dp", "tp"), None),
        P(("dp", "tp"), None),
        P("dp", "tp"),
        P("dp", "tp"),
        P("tp", "dp"),
    )

    def run(*args):
        chosen = fused_body if (mesh.shape["dp"], mesh.shape["tp"]) == (4, 8) else body
        return chosen(mesh.shape["dp"], mesh.shape["tp"], *args)

    return jax.shard_map(run, mesh=mesh, in_specs=in_specs, out_specs=out_specs, check_vma=False)
```

```python
import functools

import jax
import jax.numpy as jnp
from jax import lax
from jax.experimental import pallas as pl
from jax.experimental.pallas import tpu as pltpu
from jax.sharding import PartitionSpec as P


BF16 = jnp.bfloat16
F32 = jnp.float32


def right_trans(left, matrix):
    return lax.dot_general(left, matrix, (((1,), (1,)), ((), ())), preferred_element_type=F32)


def send_xor(block, bit, count):
    return lax.ppermute(block, "dp", [(i, i ^ bit) for i in range(count)])


def send_tp(block, dz, dx, count):
    ring = count // 2
    perm = [(i, ((i // 2 + dz) % ring) * 2 + ((i % 2) ^ dx)) for i in range(count)]
    return lax.ppermute(block, "tp", perm)


def gather_tp(own, count):
    if count != 8:
        whole = lax.all_gather(own, "tp", axis=0)
        return [whole[i] for i in range(count)]
    send = functools.partial(send_tp, count=count)
    across = send(own, 0, 1)
    below = send(own, 1, 0)
    above = send(own, -1, 0)
    across_above = send(above, 0, 1)
    across_below = send(across, 1, 0)
    far = send(above, -1, 0)
    half = own.shape[1] // 256 * 128
    left, right = across_above[:, :half], across_below[:, half:]
    left, right = send(left, -1, 0), send(right, 1, 0)
    across_far = jnp.concatenate([left, right], axis=1)
    return [own, across, above, across_above, far, across_far, below, across_below]


def scatter_tp(partial, count):
    rows = partial.shape[0] // count
    if count != 8:
        return lax.psum_scatter(partial.astype(F32), "tp", scatter_dimension=0, tiled=True).astype(BF16)
    send = functools.partial(send_tp, count=count)
    half = partial.shape[1] // 256 * 128
    near, above, far, below = (partial[i * 2 * rows : (i + 1) * 2 * rows] for i in range(4))
    left, right = far[:, :half], far[:, half:]
    from_below, from_above = send(left, 1, 0), send(right, -1, 0)
    up = jnp.concatenate(
        [(above[:, :half].astype(F32) + from_below.astype(F32)).astype(BF16), above[:, half:]], axis=1
    )
    down = jnp.concatenate(
        [below[:, :half], (below[:, half:].astype(F32) + from_above.astype(F32)).astype(BF16)], axis=1
    )
    up, down = send(up, 1, 0), send(down, -1, 0)
    total = near.astype(F32) + up.astype(F32) + down.astype(F32)
    crossed = total[rows:].astype(BF16)
    crossed = send(crossed, 0, 1)
    return (total[:rows] + crossed.astype(F32)).astype(BF16)


def gather_dp(own, count):
    blocks = {0: own}
    bit = count // 2
    while bit:
        blocks.update({k | bit: send_xor(b, bit, count) for k, b in list(blocks.items())})
        bit //= 2
    return [blocks[k] for k in range(count)]


def grad_kernel(count, *refs):
    lefts, rights, out = refs[:count], refs[count : 2 * count], refs[-1]
    total = None
    for left, right in zip(lefts, rights):
        part = lax.dot_general(
            left[...], right[...], (((0,), (0,)), ((), ())), preferred_element_type=F32
        )
        total = part if total is None else total + part
    out[...] = total


def token_sum(lefts, rights):
    count = len(lefts)
    tokens, rows = lefts[0].shape
    cols = rights[0].shape[1]
    tile = 256 if rows % 256 == 0 else 128
    return pl.pallas_call(
        functools.partial(grad_kernel, count),
        grid=(rows // tile,),
        in_specs=[pl.BlockSpec((tokens, tile), lambda i: (0, i))] * count
        + [pl.BlockSpec((tokens, cols), lambda i: (0, 0))] * count,
        out_specs=pl.BlockSpec((tile, cols), lambda i: (i, 0)),
        out_shape=jax.ShapeDtypeStruct((rows, cols), F32),
        cost_estimate=pl.CostEstimate(
            flops=2 * count * tokens * rows * cols,
            bytes_accessed=2 * count * tokens * (rows + cols) + 4 * rows * cols,
            transcendentals=0,
        ),
        compiler_params=pltpu.CompilerParams(vmem_limit_bytes=32 << 20),
    )(*lefts, *rights)


def body(dp, tp, tokens, w_gate, w_up, w_down, cotangent):
    me = lax.axis_index("dp")
    part = tokens.shape[1] // dp

    def features(x, k):
        return lax.dynamic_slice_in_dim(x, (me ^ k) * part, part, axis=1)

    gathered = jnp.concatenate(gather_tp(tokens, tp), axis=0)
    gate = jnp.dot(gathered, w_gate, preferred_element_type=F32)
    up = jnp.dot(gathered, w_up, preferred_element_type=F32)

    grads = gather_tp(cotangent, tp)
    grad_full = jnp.concatenate(grads, axis=0)

    sig = jax.nn.sigmoid(gate)
    act = gate * sig
    hidden = (act * up).astype(BF16)
    gate, up, hidden = lax.optimization_barrier((gate, up, hidden))
    mixed = jnp.dot(hidden, w_down, preferred_element_type=F32).astype(BF16)
    sig = jax.nn.sigmoid(gate)
    act = gate * sig
    back = right_trans(grad_full, w_down)
    dgate = (back * up * sig * (1.0 + gate * (1.0 - sig))).astype(BF16)
    dup = (back * act).astype(BF16)

    mixed = scatter_tp(mixed, tp)
    partial = (right_trans(dgate, w_gate) + right_trans(dup, w_up)).astype(BF16)
    input_grad = scatter_tp(partial, tp)

    token_parts = [features(gathered, 0)] + [
        send_xor(features(gathered, k), k, dp) for k in range(1, dp)
    ]

    far = [send_xor(features(cotangent, k), k, dp) for k in range(2, dp)]
    rows = cotangent.shape[0]
    far = gather_tp(jnp.concatenate(far, axis=0), tp)
    grad_parts = [features(grad_full, 0), send_xor(features(grad_full, 1), 1, dp)] + [
        jnp.concatenate([f[i * rows : (i + 1) * rows] for f in far], axis=0) for i in range(dp - 2)
    ]

    all_hidden = gather_dp(hidden, dp)
    all_dgate = gather_dp(dgate, dp)
    all_dup = gather_dp(dup, dp)
    down_grad = token_sum(all_hidden, grad_parts)
    gate_grad = token_sum(token_parts, all_dgate)
    up_grad = token_sum(token_parts, all_dup)
    return (mixed, input_grad, gate_grad, up_grad, down_grad)


MESH = pl.DeviceIdType.MESH
CORES, COLS, HALVES = 2, 2, 2


def fused_kernel(
    tokens, cotangent, w_gate, w_up, w_down,
    mixed, input_grad, features, units,
    blocks, gate, up, back, hidden, dgate, dup, partial, from_x, from_below, from_above, onward,
    edge_out, edge_in, edge_keep,
    gu_tiles, down_tiles, in_tiles,
    own_sem, gu_sem, down_sem, in_sem,
    up_send, up_recv, dn_send, dn_recv, x_send, x_recv,
    eu_send, eu_recv, ed_send, ed_recv, ee_send, ee_recv,
    ex_send, ex_recv, un_send, un_recv, un_local,
    rx_send, rx_recv, rz_send, ru_recv, rd_recv,
):
    me, place = lax.axis_index("dp"), lax.axis_index("tp")
    z, x = place // COLS, place % COLS
    y, core = me // CORES, me % CORES
    rows, _ = tokens.shape
    steps, held, part = blocks.shape[0] // 2, blocks.shape[1], blocks.shape[2]
    levels = held // rows // COLS
    column = levels * rows
    inner = gate.shape[1]
    half = inner // 2
    edge = part // 7 // 128 * 128
    main = part - edge
    ahead = 8
    top = levels - 1
    beside = (me, z * COLS + (1 - x))
    above, below = (me, place + COLS), (me, place - COLS)
    twin = y * CORES + (1 - core)
    across = (1 - y) * CORES + core

    def owner(g):
        s = lax.rem(g, steps) // HALVES
        return lax.rem(s + 1 + y, 2) * 2 + s // 2

    def at_column(g):
        return pl.multiple_of((owner(g) * HALVES + lax.rem(g, HALVES)) * part, 128)

    def remote(src, dst, send, recv, device):
        return pltpu.make_async_remote_copy(
            src_ref=src, dst_ref=dst, send_sem=send, recv_sem=recv, device_id=device, device_id_type=MESH
        )

    def spot(g, col, level, first=0, last=None):
        last = part if last is None else last
        return blocks.at[g, pl.ds(pl.multiple_of((col * levels + level) * rows, rows), rows), first:last]

    def rim(g, col, level):
        return spot(g, col, level, main, part)

    def go_up(g, h):
        ref = spot(g, x, z - h)
        return remote(ref, ref, up_send.at[g, h], up_recv.at[g, h], above)

    def go_down(g, h):
        ref = spot(g, x, z + h)
        return remote(ref, ref, dn_send.at[g, h], dn_recv.at[g, h], below)

    def rim_up(g, h):
        ref = rim(g, 1 - x, z - h)
        return remote(ref, ref, eu_send.at[g, h], eu_recv.at[g, h], above)

    def rim_down(g, h):
        ref = rim(g, 1 - x, z + h)
        return remote(ref, ref, ed_send.at[g, h], ed_recv.at[g, h], below)

    def own_x(g):
        ref = spot(g, x, z)
        return remote(ref, ref, x_send.at[g, z], x_recv.at[g, z], beside)

    def go_x(g, level):
        ref = spot(g, x, level, 0, main)
        return remote(ref, ref, x_send.at[g, level], x_recv.at[g, level], beside)

    def own(g):
        @pl.when(g < steps)
        def _():
            own_copy(g, tokens).wait()

        @pl.when(g >= steps)
        def _():
            own_copy(g, cotangent).wait()

        @pl.when(z < top)
        def _():
            go_up(g, 0).start()

        @pl.when(z > 0)
        def _():
            go_down(g, 0).start()

        own_x(g).start()
        share(g, z)

    def turn(g):
        ref = spot(g, 1 - x, z)
        remote(ref, ref, x_send.at[g, z], x_recv.at[g, z], beside).wait_recv()

        @pl.when(z < top)
        def _():
            rim_up(g, 0).start()

        @pl.when(z > 0)
        def _():
            rim_down(g, 0).start()

    def relay(g, h):
        @pl.when(z >= h)
        def _():
            ref = spot(g, x, z - h)
            remote(ref, ref, up_send.at[g, h - 1], up_recv.at[g, h - 1], below).wait_recv()
            if h < top:
                @pl.when(z < top)
                def _():
                    go_up(g, h).start()

            go_x(g, z - h).start()
            share(g, z - h)

        @pl.when(z + h <= top)
        def _():
            ref = spot(g, x, z + h)
            remote(ref, ref, dn_send.at[g, h - 1], dn_recv.at[g, h - 1], above).wait_recv()
            if h < top:
                @pl.when(z > 0)
                def _():
                    go_down(g, h).start()

            go_x(g, z + h).start()
            share(g, z + h)

    def relay_rim(g, h):
        @pl.when(z >= h)
        def _():
            ref = rim(g, 1 - x, z - h)
            remote(ref, ref, eu_send.at[g, h - 1], eu_recv.at[g, h - 1], below).wait_recv()
            if h < top:
                @pl.when(z < top)
                def _():
                    rim_up(g, h).start()

        @pl.when(z + h <= top)
        def _():
            ref = rim(g, 1 - x, z + h)
            remote(ref, ref, ed_send.at[g, h - 1], ed_recv.at[g, h - 1], above).wait_recv()
            if h < top:
                @pl.when(z > 0)
                def _():
                    rim_down(g, h).start()

    def step_in(g, lag, act):
        @pl.when((g + lag >= 0) & (g + lag < 2 * steps))
        def _():
            act(g + lag)

    def first_acts(g):
        step_in(g, ahead, own)
        step_in(g, ahead - 2, turn)
        step_in(g, ahead - 2, lambda c: relay(c, 1))
        step_in(g, ahead - 4, lambda c: relay_rim(c, 1))

    def second_acts(g):
        step_in(g, ahead - 4, lambda c: relay(c, 2))
        step_in(g, ahead - 6, lambda c: relay_rim(c, 2))

    def third_acts(g):
        step_in(g, ahead - 6, lambda c: relay(c, 3))

    def arrived(g):
        relay_rim(g, 3)
        for h in range(1, levels):
            @pl.when(z >= h)
            def _():
                ref = spot(g, 1 - x, z - h, 0, main)
                remote(ref, ref, x_send.at[g, z - h], x_recv.at[g, z - h], beside).wait_recv()

            @pl.when(z + h <= top)
            def _():
                ref = spot(g, 1 - x, z + h, 0, main)
                remote(ref, ref, x_send.at[g, z + h], x_recv.at[g, z + h], beside).wait_recv()

    def shared(g, who):
        piece = lax.rem(g, HALVES)
        return features.at[g // steps, who, :, pl.ds(pl.multiple_of(piece * part, 128), part)]

    def local_share(g):
        return pltpu.make_async_copy(blocks.at[g], shared(g, me), ex_send.at[g, 0])

    def lines_share(g, first, count, index):
        lines = pl.ds(pl.multiple_of(first, rows), count)
        recv = ex_recv.at[g // steps, me, lax.rem(g, HALVES), index]
        return remote(
            blocks.at[g, lines, :], shared(g, me).at[lines, :], ex_send.at[g, index], recv, (owner(g), place)
        )

    def block_share(g, level):
        return lines_share(g, (x * levels + level) * rows, rows, level)

    def rest_share(g):
        return lines_share(g, (1 - x) * column, column, levels)

    def share(g, level):
        @pl.when(owner(g) != me)
        def _():
            block_share(g, level).start()

    def exchange(g):
        @pl.when(owner(g) == me)
        def _():
            local_share(g).start()

        @pl.when(owner(g) != me)
        def _():
            rest_share(g).start()

    def exchange_done(g):
        @pl.when(owner(g) == me)
        def _():
            local_share(g).wait()

        @pl.when(owner(g) != me)
        def _():
            for level in range(levels):
                block_share(g, level).wait_send()
            rest_share(g).wait_send()

    def units_copies(src, k):
        dst = units.at[k, me]
        return (
            pltpu.make_async_copy(src, dst, un_local.at[k]),
            remote(src, dst, un_send.at[k, 0], un_recv.at[k, me], (across, place)),
            remote(src, dst, un_send.at[k, 1], un_recv.at[k, me], (twin, place)),
        )

    def units_forward(k):
        ref = units.at[k, across]
        return remote(ref, ref, un_send.at[k, 2], un_recv.at[k, across], (twin, place))

    def units_arrived(k, who):
        ref = units.at[k, who]
        remote(ref, ref, un_send.at[k, 2], un_recv.at[k, who], (twin, place)).wait_recv()

    def gu_copy(g, t):
        source = w_gate if t < 2 else w_up
        return pltpu.make_async_copy(
            source.at[pl.ds(at_column(g), part), (t % 2) * half : (t % 2 + 1) * half], gu_tiles.at[t], gu_sem.at[t]
        )

    def down_copy(g, t):
        slot = lax.rem(g, 2)
        return pltpu.make_async_copy(
            w_down.at[t * half : (t + 1) * half, pl.ds(at_column(g), part)],
            down_tiles.at[slot, t],
            down_sem.at[slot, t],
        )

    def in_copy(j, k):
        slot = lax.rem(j, 2)
        return pltpu.make_async_copy(
            (w_gate, w_up)[k].at[pl.ds(at_column(j), part), :], in_tiles.at[slot, k], in_sem.at[slot, k]
        )

    def rs_x(q):
        src = partial.at[q, pl.ds(pl.multiple_of((1 - x) * column, rows), column), 0:main]
        return remote(src, from_x.at[q], rx_send.at[q], rx_recv.at[q], beside)

    def rs_edge(q):
        return remote(edge_out.at[q], edge_in.at[q], ee_send.at[q], ee_recv.at[q], beside)

    def rs_up(q, first, count):
        return remote(
            onward.at[q, first * rows : (first + count) * rows, :],
            from_below.at[q, 0 : count * rows, :],
            rz_send.at[q, 0], ru_recv.at[q], above,
        )

    def rs_down(q, first, count):
        return remote(
            onward.at[q, first * rows : (first + count) * rows, :],
            from_above.at[q, 0 : count * rows, :],
            rz_send.at[q, 1], rd_recv.at[q], below,
        )

    def below_arrived(q, count):
        ref = from_below.at[q, 0 : count * rows, :]
        remote(ref, ref, rz_send.at[q, 0], ru_recv.at[q], below).wait_recv()

    def above_arrived(q, count):
        ref = from_above.at[q, 0 : count * rows, :]
        remote(ref, ref, rz_send.at[q, 1], rd_recv.at[q], above).wait_recv()

    spans = (slice(0, main), slice(main, part), slice(part, part + edge))

    def total(q, level, *more):
        near = pl.ds(pl.multiple_of(x * column + level * rows, rows), rows)
        other = pl.ds(pl.multiple_of((1 - x) * column + level * rows, rows), rows)
        values = [
            partial[q, near, 0:main].astype(F32) + from_x[q, level * rows : (level + 1) * rows, :].astype(F32),
            partial[q, near, main:part].astype(F32),
            partial[q, other, main:part].astype(F32),
        ]
        for ref, at in more:
            values = [
                value + ref[q, at * rows : (at + 1) * rows, span].astype(F32) for value, span in zip(values, spans)
            ]
        return values

    def put(q, at, values):
        for value, span in zip(values, spans):
            onward[q, at * rows : (at + 1) * rows, span] = value.astype(BF16)

    def store(q, first, value):
        cols = pl.ds(pl.multiple_of(at_column(q) + first, 128), value.shape[1])

        @pl.when(q < steps)
        def _():
            mixed[:, cols] = value

        @pl.when(q >= steps)
        def _():
            input_grad[:, cols] = value

    def emit(q, values):
        store(q, 0, values[0].astype(BF16))
        edge_keep[q] = values[1]
        edge_out[q] = values[2].astype(BF16)

    def stage_one(q):
        rs_x(q).wait_recv()

        @pl.when(z == 0)
        def _():
            for level in (1, 2, 3):
                put(q, level - 1, total(q, level))
            rs_up(q, 0, 3).start()

        @pl.when(z == 3)
        def _():
            for level in (0, 1, 2):
                put(q, level, total(q, level))
            rs_down(q, 0, 3).start()

    def stage_two(q):
        @pl.when(z == 1)
        def _():
            below_arrived(q, 3)
            for level in (2, 3):
                put(q, level - 2, total(q, level, (from_below, level - 1)))
            rs_up(q, 0, 2).start()

        @pl.when(z == 2)
        def _():
            above_arrived(q, 3)
            for level in (0, 1):
                put(q, level, total(q, level, (from_above, level)))
            rs_down(q, 0, 2).start()

    def stage_three(q):
        @pl.when(z == 2)
        def _():
            below_arrived(q, 2)
            put(q, 2, total(q, 3, (from_below, 1)))
            rs_up(q, 2, 1).start()

        @pl.when(z == 1)
        def _():
            above_arrived(q, 2)
            put(q, 2, total(q, 0, (from_above, 0)))
            rs_down(q, 2, 1).start()

    def stage_four(q):
        @pl.when(z == 0)
        def _():
            above_arrived(q, 1)
            emit(q, total(q, 0, (from_above, 0)))

        @pl.when(z == 1)
        def _():
            emit(q, total(q, 1, (from_below, 0), (from_above, 1)))

        @pl.when(z == 2)
        def _():
            emit(q, total(q, 2, (from_below, 0), (from_above, 2)))

        @pl.when(z == 3)
        def _():
            below_arrived(q, 1)
            emit(q, total(q, 3, (from_below, 0)))

        rs_edge(q).start()

    def stage_five(q):
        rs_edge(q).wait_recv()
        store(q, main, (edge_keep[q] + edge_in[q].astype(F32)).astype(BF16))

    mine = pl.ds(pl.multiple_of((x * levels + z) * rows, rows), rows)

    def own_copy(g, source):
        return pltpu.make_async_copy(
            source.at[:, pl.ds(at_column(g), part)], blocks.at[g, mine, :], own_sem.at[g]
        )

    for s in range(steps):
        own_copy(s, tokens).start()
    for s in range(steps):
        own_copy(steps + s, cotangent).start()
    for t in range(4):
        gu_copy(0, t).start()
    for t in range(2):
        down_copy(steps, t).start()
        down_copy(steps + 1, t).start()
        in_copy(0, t).start()
        in_copy(1, t).start()

    barrier = pltpu.get_barrier_semaphore()

    def greet(device):
        pl.semaphore_signal(barrier, inc=1, device_id=device, device_id_type=MESH)

    greet(beside)
    for other in (twin, across, (1 - y) * CORES + (1 - core)):
        greet((other, place))

    @pl.when(z < top)
    def _():
        greet(above)

    @pl.when(z > 0)
    def _():
        greet(below)

    @pl.when((z > 0) & (z < top))
    def _():
        pl.semaphore_wait(barrier, 6)

    @pl.when((z == 0) | (z == top))
    def _():
        pl.semaphore_wait(barrier, 5)

    @pl.loop(0, ahead)
    def _(i):
        first_acts(i - ahead)
        second_acts(i - ahead)
        third_acts(i - ahead)

    gate[...] = jnp.zeros_like(gate)
    up[...] = jnp.zeros_like(up)
    back[...] = jnp.zeros_like(back)

    @pl.loop(0, steps)
    def _(g):
        first_acts(g)
        arrived(g)
        exchange(g)
        for t in range(4):
            gu_copy(g, t).wait()
            target, at = (gate, up)[t // 2], t % 2
            target[:, at * half : (at + 1) * half] += jnp.dot(
                blocks[g], gu_tiles[t], preferred_element_type=F32
            )

            @pl.when(g < steps - 1)
            def _():
                gu_copy(g + 1, t).start()

            if t == 1:
                second_acts(g)
        third_acts(g)

    lines = 32

    @pl.loop(0, held // lines)
    def _(i):
        at = pl.ds(pl.multiple_of(i * lines, lines), lines)
        value = gate[at, :]
        hidden[at, :] = (value * jax.nn.sigmoid(value) * up[at, :]).astype(BF16)

    for copy in units_copies(hidden, 0):
        copy.start()

    @pl.loop(steps, 2 * steps)
    def _(g):
        first_acts(g)
        for t in range(2):
            down_copy(g, t).wait()
        slot = lax.rem(g, 2)
        product = jnp.dot(hidden[:, :half], down_tiles[slot, 0], preferred_element_type=F32)
        product += jnp.dot(hidden[:, half:], down_tiles[slot, 1], preferred_element_type=F32)
        partial[g - steps] = product.astype(BF16)
        second_acts(g)
        arrived(g)
        exchange(g)
        for t in range(2):
            back[:, t * half : (t + 1) * half] += right_trans(blocks[g], down_tiles[slot, t])

            @pl.when(g + 2 < 2 * steps)
            def _():
                down_copy(g + 2, t).start()
        third_acts(g)

        @pl.when(g >= steps + 2)
        def _():
            rs_x(g - steps - 2).start()

        @pl.when(g >= steps + 4)
        def _():
            stage_one(g - steps - 4)

        @pl.when(g >= steps + 6)
        def _():
            stage_two(g - steps - 6)

    @pl.loop(steps - 2, steps)
    def _(j):
        rs_x(j).start()


    @pl.loop(0, held // lines)
    def _(i):
        at = pl.ds(pl.multiple_of(i * lines, lines), lines)
        value, other, grad = gate[at, :], up[at, :], back[at, :]
        sig = jax.nn.sigmoid(value)
        dgate[at, :] = (grad * other * sig * (1.0 + value * (1.0 - sig))).astype(BF16)
        dup[at, :] = (grad * (value * sig)).astype(BF16)

    for k, source in ((1, dgate), (2, dup)):
        for copy in units_copies(source, k):
            copy.start()
    last = 2 * steps

    def later(i, lag, stage):
        @pl.when((i >= lag) & (i < last + lag))
        def _():
            stage(i - lag)

    @pl.loop(0, last + 2)
    def _(i):
        @pl.when(i < steps)
        def _():
            slot = lax.rem(i, 2)
            for k in range(2):
                in_copy(i, k).wait()
            product = right_trans(dgate[...], in_tiles[slot, 0]) + right_trans(dup[...], in_tiles[slot, 1])
            partial[i + steps] = product.astype(BF16)

            @pl.when(i + 2 < steps)
            def _():
                for k in range(2):
                    in_copy(i + 2, k).start()

            rs_x(i + steps).start()

        later(i, -4, stage_one)
        later(i, -2, stage_two)
        later(i, 0, stage_three)
        later(i, 2, stage_four)

        @pl.when(i == 2)
        def _():
            units_arrived(0, across)
            units_forward(0).start()

        @pl.when(i == last - 5)
        def _():
            units_arrived(1, across)
            units_forward(1).start()

        @pl.when(i == last - 1)
        def _():
            units_arrived(2, across)
            units_forward(2).start()

    pl.loop(0, last)(stage_five)

    @pl.loop(0, 2 * steps)
    def _(g):
        for h in range(top):
            @pl.when((z < top) & (z >= h))
            def _():
                go_up(g, h).wait_send()
                rim_up(g, h).wait_send()

            @pl.when((z > 0) & (z + h <= top))
            def _():
                go_down(g, h).wait_send()
                rim_down(g, h).wait_send()

        for h in range(1, levels):
            @pl.when(z >= h)
            def _():
                go_x(g, z - h).wait_send()

            @pl.when(z + h <= top)
            def _():
                go_x(g, z + h).wait_send()

        own_x(g).wait_send()
        exchange_done(g)
        rs_x(g).wait_send()
        rs_edge(g).wait_send()

        @pl.when(z == 0)
        def _():
            rs_up(g, 0, 3).wait_send()

        @pl.when(z == 1)
        def _():
            rs_up(g, 0, 2).wait_send()
            rs_down(g, 2, 1).wait_send()

        @pl.when(z == 2)
        def _():
            rs_up(g, 2, 1).wait_send()
            rs_down(g, 0, 2).wait_send()

        @pl.when(z == 3)
        def _():
            rs_down(g, 0, 3).wait_send()

    for kind in range(2):
        for other in (twin, across, (1 - y) * CORES + (1 - core)):
            for piece in range(HALVES):
                for level in range(levels + 1):
                    first, size = (x * levels + level) * rows, rows
                    if level == levels:
                        first, size = (1 - x) * column, column
                    lines = pl.ds(pl.multiple_of(first, rows), size)
                    ref = features.at[kind, other, lines, piece * part : (piece + 1) * part]
                    recv = ex_recv.at[kind, other, piece, level]
                    remote(ref, ref, ex_send.at[0, level], recv, (twin, place)).wait_recv()
    for k, source in enumerate((hidden, dgate, dup)):
        local, far, near = units_copies(source, k)
        local.wait()
        far.wait_send()
        near.wait_send()
        units_forward(k).wait_send()
        units_arrived(k, twin)
        units_arrived(k, (1 - y) * CORES + (1 - core))


def fused_body(dp, tp, tokens, w_gate, w_up, w_down, cotangent):
    rows, width = tokens.shape
    inner = w_gate.shape[1]
    held, part = rows * tp, width // dp
    levels = tp // COLS
    half, sub, count = inner // 2, part // HALVES, HALVES * dp
    edge = sub // 7 // 128 * 128
    main = sub - edge
    hbm, vmem = pl.BlockSpec(memory_space=pl.ANY), pl.BlockSpec(memory_space=pltpu.VMEM)
    dma = pltpu.SemaphoreType.DMA
    chain = (levels - 1) * rows
    mixed, input_grad, features, units = pl.pallas_call(
        fused_kernel,
        in_specs=[hbm] * 5,
        out_specs=[vmem, vmem, hbm, hbm],
        out_shape=[
            jax.ShapeDtypeStruct((rows, width), BF16),
            jax.ShapeDtypeStruct((rows, width), BF16),
            jax.ShapeDtypeStruct((2, dp, held, part), BF16),
            jax.ShapeDtypeStruct((3, dp, held, inner), BF16),
        ],
        scratch_shapes=[
            pltpu.VMEM((2 * count, held, sub), BF16),
            pltpu.VMEM((held, inner), F32),
            pltpu.VMEM((held, inner), F32),
            pltpu.VMEM((held, inner), F32),
            pltpu.VMEM((held, inner), BF16),
            pltpu.VMEM((held, inner), BF16),
            pltpu.VMEM((held, inner), BF16),
            pltpu.VMEM((2 * count, held, sub), BF16),
            pltpu.VMEM((2 * count, levels * rows, main), BF16),
            pltpu.VMEM((2 * count, chain, sub + edge), BF16),
            pltpu.VMEM((2 * count, chain, sub + edge), BF16),
            pltpu.VMEM((2 * count, chain, sub + edge), BF16),
            pltpu.VMEM((2 * count, rows, edge), BF16),
            pltpu.VMEM((2 * count, rows, edge), BF16),
            pltpu.VMEM((2 * count, rows, edge), F32),
            pltpu.VMEM((4, sub, half), BF16),
            pltpu.VMEM((2, 2, half, sub), BF16),
            pltpu.VMEM((2, 2, sub, inner), BF16),
            dma((2 * count,)), dma((4,)), dma((2, 2)), dma((2, 2)),
            dma((2 * count, 3)), dma((2 * count, 3)), dma((2 * count, 3)), dma((2 * count, 3)),
            dma((2 * count, levels)), dma((2 * count, levels)),
            dma((2 * count, 3)), dma((2 * count, 3)), dma((2 * count, 3)), dma((2 * count, 3)),
            dma((2 * count,)), dma((2 * count,)),
            dma((2 * count, levels + 1)), dma((2, dp, HALVES, levels + 1)),
            dma((3, 3)), dma((3, dp)), dma((3,)),
            dma((2 * count,)), dma((2 * count,)), dma((2 * count, 2)), dma((2 * count,)), dma((2 * count,)),
        ],
        compiler_params=pltpu.CompilerParams(
            collective_id=0, has_side_effects=True, vmem_limit_bytes=67_043_328
        ),
        name="fused",
    )(tokens, cotangent, w_gate, w_up, w_down)

    tile = 256 if part % 256 == 0 and inner % 256 == 0 else 128
    early, late = inner // tile, part // tile
    depth = dp * held

    def grads(hidden_ref, cot_ref, tok_ref, units_ref, mixed_ref, in_ref, down, gate, up, mixed_out, in_out, both, sem):
        step = pl.program_id(0)

        def fetch(k):
            return pltpu.make_async_copy(units_ref.at[1 + k], both.at[k], sem.at[k])

        def product(left, right):
            return lax.dot_general(
                left.reshape(depth, left.shape[-1]),
                right.reshape(depth, right.shape[-1]),
                (((0,), (0,)), ((), ())),
                preferred_element_type=F32,
            )

        @pl.when(step == 0)
        def _():
            for k in range(2):
                fetch(k).start()
            mixed_out[...] = mixed_ref[...]
            in_out[...] = in_ref[...]

        @pl.when(step < early)
        def _():
            down[...] = product(hidden_ref[...], cot_ref[...])

        @pl.when(step == early)
        def _():
            for k in range(2):
                fetch(k).wait()

        @pl.when(step >= early)
        def _():
            gate[...] = product(tok_ref[...], both[0])
            up[...] = product(tok_ref[...], both[1])

    whole = pl.BlockSpec((rows, width), lambda i: (0, 0))

    def first(i):
        return jnp.minimum(i, early - 1)

    def second(i):
        return jnp.maximum(i - early, 0)

    down_grad, gate_grad, up_grad, mixed, input_grad = pl.pallas_call(
        grads,
        grid=(early + late,),
        in_specs=[
            pl.BlockSpec((None, dp, held, tile), lambda i: (0, 0, 0, first(i))),
            pl.BlockSpec((None, dp, held, part), lambda i: (1, 0, 0, 0)),
            pl.BlockSpec((None, dp, held, tile), lambda i: (0, 0, 0, second(i))),
            hbm,
            whole,
            whole,
        ],
        out_specs=[
            pl.BlockSpec((tile, part), lambda i: (first(i), 0)),
            pl.BlockSpec((tile, inner), lambda i: (second(i), 0)),
            pl.BlockSpec((tile, inner), lambda i: (second(i), 0)),
            whole,
            whole,
        ],
        out_shape=[
            jax.ShapeDtypeStruct((inner, part), F32),
            jax.ShapeDtypeStruct((part, inner), F32),
            jax.ShapeDtypeStruct((part, inner), F32),
            jax.ShapeDtypeStruct((rows, width), BF16),
            jax.ShapeDtypeStruct((rows, width), BF16),
        ],
        scratch_shapes=[pltpu.VMEM((2, dp, held, inner), BF16), dma((2,))],
        compiler_params=pltpu.CompilerParams(vmem_limit_bytes=60 << 20),
        name="grads",
    )(units, features, features, units, mixed, input_grad)
    return mixed, input_grad, gate_grad, up_grad, down_grad


def solution(mesh):
    in_specs = (
        P(("dp", "tp"), None),
        P(None, "tp"),
        P(None, "tp"),
        P("tp", None),
        P(("dp", "tp"), None),
    )
    out_specs = (
        P(("dp", "tp"), None),
        P(("dp", "tp"), None),
        P("dp", "tp"),
        P("dp", "tp"),
        P("tp", "dp"),
    )

    def run(*args):
        chosen = fused_body if (mesh.shape["dp"], mesh.shape["tp"]) == (4, 8) else body
        return chosen(mesh.shape["dp"], mesh.shape["tp"], *args)

    return jax.shard_map(run, mesh=mesh, in_specs=in_specs, out_specs=out_specs, check_vma=False)
```

```python
import functools

import jax
import jax.numpy as jnp
from jax import lax
from jax.experimental import pallas as pl
from jax.experimental.pallas import tpu as pltpu
from jax.sharding import PartitionSpec as P


BF16 = jnp.bfloat16
F32 = jnp.float32


def right_trans(left, matrix):
    return lax.dot_general(left, matrix, (((1,), (1,)), ((), ())), preferred_element_type=F32)


def send_xor(block, bit, count):
    return lax.ppermute(block, "dp", [(i, i ^ bit) for i in range(count)])


def send_tp(block, dz, dx, count):
    ring = count // 2
    perm = [(i, ((i // 2 + dz) % ring) * 2 + ((i % 2) ^ dx)) for i in range(count)]
    return lax.ppermute(block, "tp", perm)


def gather_tp(own, count):
    if count != 8:
        whole = lax.all_gather(own, "tp", axis=0)
        return [whole[i] for i in range(count)]
    send = functools.partial(send_tp, count=count)
    across = send(own, 0, 1)
    below = send(own, 1, 0)
    above = send(own, -1, 0)
    across_above = send(above, 0, 1)
    across_below = send(across, 1, 0)
    far = send(above, -1, 0)
    half = own.shape[1] // 256 * 128
    left, right = across_above[:, :half], across_below[:, half:]
    left, right = send(left, -1, 0), send(right, 1, 0)
    across_far = jnp.concatenate([left, right], axis=1)
    return [own, across, above, across_above, far, across_far, below, across_below]


def scatter_tp(partial, count):
    rows = partial.shape[0] // count
    if count != 8:
        return lax.psum_scatter(partial.astype(F32), "tp", scatter_dimension=0, tiled=True).astype(BF16)
    send = functools.partial(send_tp, count=count)
    half = partial.shape[1] // 256 * 128
    near, above, far, below = (partial[i * 2 * rows : (i + 1) * 2 * rows] for i in range(4))
    left, right = far[:, :half], far[:, half:]
    from_below, from_above = send(left, 1, 0), send(right, -1, 0)
    up = jnp.concatenate(
        [(above[:, :half].astype(F32) + from_below.astype(F32)).astype(BF16), above[:, half:]], axis=1
    )
    down = jnp.concatenate(
        [below[:, :half], (below[:, half:].astype(F32) + from_above.astype(F32)).astype(BF16)], axis=1
    )
    up, down = send(up, 1, 0), send(down, -1, 0)
    total = near.astype(F32) + up.astype(F32) + down.astype(F32)
    crossed = total[rows:].astype(BF16)
    crossed = send(crossed, 0, 1)
    return (total[:rows] + crossed.astype(F32)).astype(BF16)


def gather_dp(own, count):
    blocks = {0: own}
    bit = count // 2
    while bit:
        blocks.update({k | bit: send_xor(b, bit, count) for k, b in list(blocks.items())})
        bit //= 2
    return [blocks[k] for k in range(count)]


def grad_kernel(count, *refs):
    lefts, rights, out = refs[:count], refs[count : 2 * count], refs[-1]
    total = None
    for left, right in zip(lefts, rights):
        part = lax.dot_general(
            left[...], right[...], (((0,), (0,)), ((), ())), preferred_element_type=F32
        )
        total = part if total is None else total + part
    out[...] = total


def token_sum(lefts, rights):
    count = len(lefts)
    tokens, rows = lefts[0].shape
    cols = rights[0].shape[1]
    tile = 256 if rows % 256 == 0 else 128
    return pl.pallas_call(
        functools.partial(grad_kernel, count),
        grid=(rows // tile,),
        in_specs=[pl.BlockSpec((tokens, tile), lambda i: (0, i))] * count
        + [pl.BlockSpec((tokens, cols), lambda i: (0, 0))] * count,
        out_specs=pl.BlockSpec((tile, cols), lambda i: (i, 0)),
        out_shape=jax.ShapeDtypeStruct((rows, cols), F32),
        cost_estimate=pl.CostEstimate(
            flops=2 * count * tokens * rows * cols,
            bytes_accessed=2 * count * tokens * (rows + cols) + 4 * rows * cols,
            transcendentals=0,
        ),
        compiler_params=pltpu.CompilerParams(vmem_limit_bytes=32 << 20),
    )(*lefts, *rights)


def body(dp, tp, tokens, w_gate, w_up, w_down, cotangent):
    me = lax.axis_index("dp")
    part = tokens.shape[1] // dp

    def features(x, k):
        return lax.dynamic_slice_in_dim(x, (me ^ k) * part, part, axis=1)

    gathered = jnp.concatenate(gather_tp(tokens, tp), axis=0)
    gate = jnp.dot(gathered, w_gate, preferred_element_type=F32)
    up = jnp.dot(gathered, w_up, preferred_element_type=F32)

    grads = gather_tp(cotangent, tp)
    grad_full = jnp.concatenate(grads, axis=0)

    sig = jax.nn.sigmoid(gate)
    act = gate * sig
    hidden = (act * up).astype(BF16)
    gate, up, hidden = lax.optimization_barrier((gate, up, hidden))
    mixed = jnp.dot(hidden, w_down, preferred_element_type=F32).astype(BF16)
    sig = jax.nn.sigmoid(gate)
    act = gate * sig
    back = right_trans(grad_full, w_down)
    dgate = (back * up * sig * (1.0 + gate * (1.0 - sig))).astype(BF16)
    dup = (back * act).astype(BF16)

    mixed = scatter_tp(mixed, tp)
    partial = (right_trans(dgate, w_gate) + right_trans(dup, w_up)).astype(BF16)
    input_grad = scatter_tp(partial, tp)

    token_parts = [features(gathered, 0)] + [
        send_xor(features(gathered, k), k, dp) for k in range(1, dp)
    ]

    far = [send_xor(features(cotangent, k), k, dp) for k in range(2, dp)]
    rows = cotangent.shape[0]
    far = gather_tp(jnp.concatenate(far, axis=0), tp)
    grad_parts = [features(grad_full, 0), send_xor(features(grad_full, 1), 1, dp)] + [
        jnp.concatenate([f[i * rows : (i + 1) * rows] for f in far], axis=0) for i in range(dp - 2)
    ]

    all_hidden = gather_dp(hidden, dp)
    all_dgate = gather_dp(dgate, dp)
    all_dup = gather_dp(dup, dp)
    down_grad = token_sum(all_hidden, grad_parts)
    gate_grad = token_sum(token_parts, all_dgate)
    up_grad = token_sum(token_parts, all_dup)
    return (mixed, input_grad, gate_grad, up_grad, down_grad)


MESH = pl.DeviceIdType.MESH
CORES, COLS, HALVES, GATHER_EDGES, AHEAD = 2, 2, 2, 1, 8


def fused_kernel(
    tokens, cotangent, w_gate, w_up, w_down,
    mixed, input_grad, features, units,
    blocks, gate, up, back, hidden, dgate, dup, partial, from_x, from_below, from_above, onward,
    edge_out, edge_in, edge_keep,
    gu_tiles, down_tiles, in_tiles,
    own_sem, gu_sem, down_sem, in_sem,
    up_send, up_recv, dn_send, dn_recv, x_send, x_recv,
    eu_send, eu_recv, ed_send, ed_recv, ee_send, ee_recv,
    ex_send, ex_recv, un_send, un_recv, un_local,
    rx_send, rx_recv, rz_send, ru_recv, rd_recv,
):
    me, place = lax.axis_index("dp"), lax.axis_index("tp")
    z, x = place // COLS, place % COLS
    y, core = me // CORES, me % CORES
    rows, _ = tokens.shape
    steps, held, part = blocks.shape[0] // 2, blocks.shape[1], blocks.shape[2]
    levels = held // rows // COLS
    column = levels * rows
    inner = gate.shape[1]
    half = inner // 2
    edge = part // 7 // 128 * 128
    main = part - edge
    bulk = part - GATHER_EDGES * edge
    ahead = AHEAD
    top = levels - 1
    beside = (me, z * COLS + (1 - x))
    above, below = (me, place + COLS), (me, place - COLS)
    twin = y * CORES + (1 - core)
    across = (1 - y) * CORES + core

    def owner(g):
        s = lax.rem(g, steps) // HALVES
        return lax.rem(s + 1 + y, 2) * 2 + s // 2

    def at_column(g):
        return pl.multiple_of((owner(g) * HALVES + lax.rem(g, HALVES)) * part, 128)

    def remote(src, dst, send, recv, device):
        return pltpu.make_async_remote_copy(
            src_ref=src, dst_ref=dst, send_sem=send, recv_sem=recv, device_id=device, device_id_type=MESH
        )

    def spot(g, col, level, first=0, last=None):
        last = part if last is None else last
        return blocks.at[g, pl.ds(pl.multiple_of((col * levels + level) * rows, rows), rows), first:last]

    def rim(g, col, level):
        return spot(g, col, level, bulk, part)

    def go_up(g, h):
        ref = spot(g, x, z - h)
        return remote(ref, ref, up_send.at[h], up_recv.at[g, h], above)

    def go_down(g, h):
        ref = spot(g, x, z + h)
        return remote(ref, ref, dn_send.at[h], dn_recv.at[g, h], below)

    def rim_up(g, h):
        ref = rim(g, 1 - x, z - h)
        return remote(ref, ref, eu_send.at[h], eu_recv.at[g, h], above)

    def rim_down(g, h):
        ref = rim(g, 1 - x, z + h)
        return remote(ref, ref, ed_send.at[h], ed_recv.at[g, h], below)

    def own_x(g):
        ref = spot(g, x, z)
        return remote(ref, ref, x_send.at[levels], x_recv.at[g, z], beside)

    def go_x(g, level):
        ref = spot(g, x, level, 0, bulk)
        return remote(ref, ref, x_send.at[level], x_recv.at[g, level], beside)

    def own(g):
        @pl.when(g < steps)
        def _():
            own_copy(g, tokens).wait()

        @pl.when(g >= steps)
        def _():
            own_copy(g, cotangent).wait()

        @pl.when(z < top)
        def _():
            go_up(g, 0).start()

        @pl.when(z > 0)
        def _():
            go_down(g, 0).start()

        own_x(g).start()
        share(g, z)

    def turn(g):
        ref = spot(g, 1 - x, z)
        remote(ref, ref, x_send.at[levels], x_recv.at[g, z], beside).wait_recv()

        @pl.when(z < top)
        def _():
            rim_up(g, 0).start()

        @pl.when(z > 0)
        def _():
            rim_down(g, 0).start()

    def relay(g, h):
        @pl.when(z >= h)
        def _():
            ref = spot(g, x, z - h)
            remote(ref, ref, up_send.at[h - 1], up_recv.at[g, h - 1], below).wait_recv()
            if h < top:
                @pl.when(z < top)
                def _():
                    go_up(g, h).start()

            go_x(g, z - h).start()
            share(g, z - h)

        @pl.when(z + h <= top)
        def _():
            ref = spot(g, x, z + h)
            remote(ref, ref, dn_send.at[h - 1], dn_recv.at[g, h - 1], above).wait_recv()
            if h < top:
                @pl.when(z > 0)
                def _():
                    go_down(g, h).start()

            go_x(g, z + h).start()
            share(g, z + h)

    def relay_rim(g, h):
        @pl.when(z >= h)
        def _():
            ref = rim(g, 1 - x, z - h)
            remote(ref, ref, eu_send.at[h - 1], eu_recv.at[g, h - 1], below).wait_recv()
            if h < top:
                @pl.when(z < top)
                def _():
                    rim_up(g, h).start()

        @pl.when(z + h <= top)
        def _():
            ref = rim(g, 1 - x, z + h)
            remote(ref, ref, ed_send.at[h - 1], ed_recv.at[g, h - 1], above).wait_recv()
            if h < top:
                @pl.when(z > 0)
                def _():
                    rim_down(g, h).start()

    def step_in(g, lag, act):
        @pl.when((g + lag >= 0) & (g + lag < 2 * steps))
        def _():
            act(g + lag)

    def first_acts(g):
        step_in(g, ahead, own)
        step_in(g, ahead - 2, turn)
        step_in(g, ahead - 2, lambda c: relay(c, 1))
        step_in(g, ahead - 4, lambda c: relay_rim(c, 1))

    def second_acts(g):
        step_in(g, ahead - 4, lambda c: relay(c, 2))
        step_in(g, ahead - 6, lambda c: relay_rim(c, 2))

    def third_acts(g):
        step_in(g, ahead - 6, lambda c: relay(c, 3))

    def arrived(g):
        relay_rim(g, 3)
        for h in range(1, levels):
            @pl.when(z >= h)
            def _():
                ref = spot(g, 1 - x, z - h, 0, bulk)
                remote(ref, ref, x_send.at[z - h], x_recv.at[g, z - h], beside).wait_recv()

            @pl.when(z + h <= top)
            def _():
                ref = spot(g, 1 - x, z + h, 0, bulk)
                remote(ref, ref, x_send.at[z + h], x_recv.at[g, z + h], beside).wait_recv()

    def shared(g, who):
        piece = lax.rem(g, HALVES)
        return features.at[g // steps, who, :, pl.ds(pl.multiple_of(piece * part, 128), part)]

    def local_share(g):
        return pltpu.make_async_copy(blocks.at[g], shared(g, me), ex_send.at[levels + 1])

    def lines_share(g, first, count, index):
        lines = pl.ds(pl.multiple_of(first, rows), count)
        recv = ex_recv.at[g // steps, me, lax.rem(g, HALVES), index]
        return remote(
            blocks.at[g, lines, :], shared(g, me).at[lines, :], ex_send.at[index], recv, (owner(g), place)
        )

    def block_share(g, level):
        return lines_share(g, (x * levels + level) * rows, rows, level)

    def rest_share(g):
        return lines_share(g, (1 - x) * column, column, levels)

    def share(g, level):
        @pl.when(owner(g) != me)
        def _():
            block_share(g, level).start()

    def exchange(g):
        @pl.when(owner(g) == me)
        def _():
            local_share(g).start()

        @pl.when(owner(g) != me)
        def _():
            rest_share(g).start()

    def units_copies(src, k):
        dst = units.at[k, me]
        return (
            pltpu.make_async_copy(src, dst, un_local.at[k]),
            remote(src, dst, un_send.at[k, 0], un_recv.at[k, me], (across, place)),
            remote(src, dst, un_send.at[k, 1], un_recv.at[k, me], (twin, place)),
        )

    def units_forward(k):
        ref = units.at[k, across]
        return remote(ref, ref, un_send.at[k, 2], un_recv.at[k, across], (twin, place))

    def units_arrived(k, who):
        ref = units.at[k, who]
        remote(ref, ref, un_send.at[k, 2], un_recv.at[k, who], (twin, place)).wait_recv()

    def gu_copy(g, t):
        source = w_gate if t < 2 else w_up
        return pltpu.make_async_copy(
            source.at[pl.ds(at_column(g), part), (t % 2) * half : (t % 2 + 1) * half], gu_tiles.at[t], gu_sem.at[t]
        )

    def down_copy(g, t):
        slot = lax.rem(g, 2)
        return pltpu.make_async_copy(
            w_down.at[t * half : (t + 1) * half, pl.ds(at_column(g), part)],
            down_tiles.at[slot, t],
            down_sem.at[slot, t],
        )

    def in_copy(j, k):
        slot = lax.rem(j, 2)
        return pltpu.make_async_copy(
            (w_gate, w_up)[k].at[pl.ds(at_column(j), part), :], in_tiles.at[slot, k], in_sem.at[slot, k]
        )

    def rs_x(q):
        src = partial.at[q, pl.ds(pl.multiple_of((1 - x) * column, rows), column), 0:main]
        return remote(src, from_x.at[q], rx_send.at[0], rx_recv.at[q], beside)

    def rs_edge(q):
        return remote(edge_out.at[q], edge_in.at[q], ee_send.at[0], ee_recv.at[q], beside)

    def slot(ref, q, at):
        return ref.at[q, at * rows : (at + 1) * rows, :]

    def rs_up(q, level):
        at = level - 1
        return remote(
            slot(onward, q, at), slot(from_below, q, at), rz_send.at[at], ru_recv.at[q, at], above
        )

    def rs_down(q, level):
        return remote(
            slot(onward, q, level), slot(from_above, q, level), rz_send.at[level], rd_recv.at[q, level], below
        )

    def below_arrived(q, level):
        ref = slot(from_below, q, level - 1)
        remote(ref, ref, rz_send.at[level - 1], ru_recv.at[q, level - 1], below).wait_recv()

    def above_arrived(q, level):
        ref = slot(from_above, q, level)
        remote(ref, ref, rz_send.at[level], rd_recv.at[q, level], above).wait_recv()

    spans = (slice(0, main), slice(main, part), slice(part, part + edge))

    def total(q, level, *more):
        near = pl.ds(pl.multiple_of(x * column + level * rows, rows), rows)
        other = pl.ds(pl.multiple_of((1 - x) * column + level * rows, rows), rows)
        values = [
            partial[q, near, 0:main].astype(F32) + from_x[q, level * rows : (level + 1) * rows, :].astype(F32),
            partial[q, near, main:part].astype(F32),
            partial[q, other, main:part].astype(F32),
        ]
        for ref, at in more:
            values = [
                value + ref[q, at * rows : (at + 1) * rows, span].astype(F32) for value, span in zip(values, spans)
            ]
        return values

    def put(q, at, values):
        for value, span in zip(values, spans):
            onward[q, at * rows : (at + 1) * rows, span] = value.astype(BF16)

    def store(q, first, value):
        cols = pl.ds(pl.multiple_of(at_column(q) + first, 128), value.shape[1])

        @pl.when(q < steps)
        def _():
            mixed[:, cols] = value

        @pl.when(q >= steps)
        def _():
            input_grad[:, cols] = value

    def emit(q, values):
        store(q, 0, values[0].astype(BF16))
        edge_keep[q] = values[1]
        edge_out[q] = values[2].astype(BF16)

    def up_with(q, level, *more):
        put(q, level - 1, total(q, level, *more))
        rs_up(q, level).start()

    def down_with(q, level, *more):
        put(q, level, total(q, level, *more))
        rs_down(q, level).start()

    def stage_one(q):
        rs_x(q).wait_recv()

        @pl.when(z == 0)
        def _():
            for level in (3, 2, 1):
                up_with(q, level)

        @pl.when(z == 3)
        def _():
            for level in (0, 1, 2):
                down_with(q, level)

    def stage_two(q):
        @pl.when(z == 1)
        def _():
            for level in (3, 2):
                below_arrived(q, level)
                up_with(q, level, (from_below, level - 1))

        @pl.when(z == 2)
        def _():
            for level in (0, 1):
                above_arrived(q, level)
                down_with(q, level, (from_above, level))

    def stage_three(q):
        @pl.when(z == 2)
        def _():
            below_arrived(q, 3)
            up_with(q, 3, (from_below, 2))

        @pl.when(z == 1)
        def _():
            above_arrived(q, 0)
            down_with(q, 0, (from_above, 0))

    def stage_four(q):
        @pl.when(z == 0)
        def _():
            above_arrived(q, 0)
            emit(q, total(q, 0, (from_above, 0)))

        @pl.when(z == 1)
        def _():
            below_arrived(q, 1)
            above_arrived(q, 1)
            emit(q, total(q, 1, (from_below, 0), (from_above, 1)))

        @pl.when(z == 2)
        def _():
            below_arrived(q, 2)
            above_arrived(q, 2)
            emit(q, total(q, 2, (from_below, 1), (from_above, 2)))

        @pl.when(z == 3)
        def _():
            below_arrived(q, 3)
            emit(q, total(q, 3, (from_below, 2)))

        rs_edge(q).start()

    def stage_five(q):
        rs_edge(q).wait_recv()
        store(q, main, (edge_keep[q] + edge_in[q].astype(F32)).astype(BF16))

    def sent(ref, sem):
        remote(ref, ref, sem, rx_recv.at[0], beside).wait_send()

    def lines_of(col, level, first=0, last=None):
        start = pl.multiple_of((col * levels + level) * rows, rows)
        return blocks.at[:, pl.ds(start, rows), first : part if last is None else last]

    barrier = pltpu.get_barrier_semaphore()

    def greet(device):
        pl.semaphore_signal(barrier, inc=1, device_id=device, device_id_type=MESH)

    greet(beside)
    for other in (twin, across, (1 - y) * CORES + (1 - core)):
        greet((other, place))

    @pl.when(z < top)
    def _():
        greet(above)

    @pl.when(z > 0)
    def _():
        greet(below)

    mine = pl.ds(pl.multiple_of((x * levels + z) * rows, rows), rows)

    def own_copy(g, source):
        return pltpu.make_async_copy(
            source.at[:, pl.ds(at_column(g), part)], blocks.at[g, mine, :], own_sem.at[g]
        )

    for s in range(steps):
        own_copy(s, tokens).start()
    for s in range(steps):
        own_copy(steps + s, cotangent).start()
    for t in range(4):
        gu_copy(0, t).start()
    for t in range(2):
        down_copy(steps, t).start()
        down_copy(steps + 1, t).start()
        in_copy(0, t).start()
        in_copy(1, t).start()

    @pl.when((z > 0) & (z < top))
    def _():
        pl.semaphore_wait(barrier, 6)

    @pl.when((z == 0) | (z == top))
    def _():
        pl.semaphore_wait(barrier, 5)

    @pl.loop(0, ahead)
    def _(i):
        first_acts(i - ahead)
        second_acts(i - ahead)
        third_acts(i - ahead)

    gate[...] = jnp.zeros_like(gate)
    up[...] = jnp.zeros_like(up)
    back[...] = jnp.zeros_like(back)

    @pl.loop(0, steps)
    def _(g):
        first_acts(g)
        arrived(g)
        exchange(g)
        for t in range(4):
            gu_copy(g, t).wait()
            target, at = (gate, up)[t // 2], t % 2
            target[:, at * half : (at + 1) * half] += jnp.dot(
                blocks[g], gu_tiles[t], preferred_element_type=F32
            )

            @pl.when(g < steps - 1)
            def _():
                gu_copy(g + 1, t).start()

            if t == 1:
                second_acts(g)
        third_acts(g)

    lines = 32

    @pl.loop(0, held // lines)
    def _(i):
        at = pl.ds(pl.multiple_of(i * lines, lines), lines)
        value = gate[at, :]
        hidden[at, :] = (value * jax.nn.sigmoid(value) * up[at, :]).astype(BF16)

    for copy in units_copies(hidden, 0):
        copy.start()

    @pl.loop(steps, 2 * steps)
    def _(g):
        first_acts(g)
        for t in range(2):
            down_copy(g, t).wait()
        slot = lax.rem(g, 2)
        product = jnp.dot(hidden[:, :half], down_tiles[slot, 0], preferred_element_type=F32)
        product += jnp.dot(hidden[:, half:], down_tiles[slot, 1], preferred_element_type=F32)
        partial[g - steps] = product.astype(BF16)
        second_acts(g)
        arrived(g)
        exchange(g)
        for t in range(2):
            back[:, t * half : (t + 1) * half] += right_trans(blocks[g], down_tiles[slot, t])

            @pl.when(g + 2 < 2 * steps)
            def _():
                down_copy(g + 2, t).start()
        third_acts(g)

        @pl.when(g >= steps + 2)
        def _():
            rs_x(g - steps - 2).start()

        @pl.when(g >= steps + 4)
        def _():
            stage_one(g - steps - 4)

        @pl.when(g >= steps + 6)
        def _():
            stage_two(g - steps - 6)

    @pl.loop(steps - 2, steps)
    def _(j):
        rs_x(j).start()


    @pl.loop(0, held // lines)
    def _(i):
        at = pl.ds(pl.multiple_of(i * lines, lines), lines)
        value, other, grad = gate[at, :], up[at, :], back[at, :]
        sig = jax.nn.sigmoid(value)
        dgate[at, :] = (grad * other * sig * (1.0 + value * (1.0 - sig))).astype(BF16)
        dup[at, :] = (grad * (value * sig)).astype(BF16)

    for k, source in ((1, dgate), (2, dup)):
        for copy in units_copies(source, k):
            copy.start()
    last = 2 * steps

    def later(i, lag, stage):
        @pl.when((i >= lag) & (i < last + lag))
        def _():
            stage(i - lag)

    @pl.loop(0, last + 2)
    def _(i):
        @pl.when(i < steps)
        def _():
            slot = lax.rem(i, 2)
            for k in range(2):
                in_copy(i, k).wait()
            product = right_trans(dgate[...], in_tiles[slot, 0]) + right_trans(dup[...], in_tiles[slot, 1])
            partial[i + steps] = product.astype(BF16)

            @pl.when(i + 2 < steps)
            def _():
                for k in range(2):
                    in_copy(i + 2, k).start()

            rs_x(i + steps).start()

        later(i, -4, stage_one)
        later(i, -2, stage_two)
        later(i, 0, stage_three)
        later(i, 2, stage_four)

        @pl.when(i == 2)
        def _():
            units_arrived(0, across)
            units_forward(0).start()

        @pl.when(i == last - 5)
        def _():
            units_arrived(1, across)
            units_forward(1).start()

        @pl.when(i == last - 1)
        def _():
            units_arrived(2, across)
            units_forward(2).start()

    pl.loop(0, last)(stage_five)

    for h in range(top):
        @pl.when((z < top) & (z >= h))
        def _():
            sent(lines_of(x, z - h), up_send.at[h])
            sent(lines_of(1 - x, z - h, bulk), eu_send.at[h])

        @pl.when((z > 0) & (z + h <= top))
        def _():
            sent(lines_of(x, z + h), dn_send.at[h])
            sent(lines_of(1 - x, z + h, bulk), ed_send.at[h])

    for h in range(1, levels):
        @pl.when(z >= h)
        def _():
            sent(lines_of(x, z - h, 0, bulk), x_send.at[z - h])

        @pl.when(z + h <= top)
        def _():
            sent(lines_of(x, z + h, 0, bulk), x_send.at[z + h])

    sent(lines_of(x, z), x_send.at[levels])
    parts = steps // HALVES
    remotes, locals_ = 2 * steps // parts * (parts - 1), 2 * steps // parts
    for level in range(levels):
        start = pl.multiple_of((x * levels + level) * rows, rows)
        sent(blocks.at[0:remotes, pl.ds(start, rows), :], ex_send.at[level])
    start = pl.multiple_of((1 - x) * column, rows)
    sent(blocks.at[0:remotes, pl.ds(start, column), :], ex_send.at[levels])
    same = blocks.at[0:locals_]
    pltpu.make_async_copy(same, same, ex_send.at[levels + 1]).wait()
    sent(partial.at[:, pl.ds(start, column), 0:main], rx_send.at[0])
    for at in range(top):
        sent(onward.at[:, at * rows : (at + 1) * rows, :], rz_send.at[at])
    sent(edge_out, ee_send.at[0])

    for kind in range(2):
        for other in (twin, across, (1 - y) * CORES + (1 - core)):
            for piece in range(HALVES):
                for level in range(levels + 1):
                    first, size = (x * levels + level) * rows, rows
                    if level == levels:
                        first, size = (1 - x) * column, column
                    lines = pl.ds(pl.multiple_of(first, rows), size)
                    ref = features.at[kind, other, lines, piece * part : (piece + 1) * part]
                    recv = ex_recv.at[kind, other, piece, level]
                    remote(ref, ref, ex_send.at[level], recv, (twin, place)).wait_recv()
    for k, source in enumerate((hidden, dgate, dup)):
        local, far, near = units_copies(source, k)
        local.wait()
        far.wait_send()
        near.wait_send()
        units_forward(k).wait_send()
        units_arrived(k, twin)
        units_arrived(k, (1 - y) * CORES + (1 - core))


def fused_body(dp, tp, tokens, w_gate, w_up, w_down, cotangent):
    rows, width = tokens.shape
    inner = w_gate.shape[1]
    held, part = rows * tp, width // dp
    levels = tp // COLS
    half, sub, count = inner // 2, part // HALVES, HALVES * dp
    edge = sub // 7 // 128 * 128
    main = sub - edge
    hbm, vmem = pl.BlockSpec(memory_space=pl.ANY), pl.BlockSpec(memory_space=pltpu.VMEM)
    dma = pltpu.SemaphoreType.DMA
    chain = (levels - 1) * rows
    mixed, input_grad, features, units = pl.pallas_call(
        fused_kernel,
        in_specs=[hbm] * 5,
        out_specs=[vmem, vmem, hbm, hbm],
        out_shape=[
            jax.ShapeDtypeStruct((rows, width), BF16),
            jax.ShapeDtypeStruct((rows, width), BF16),
            jax.ShapeDtypeStruct((2, dp, held, part), BF16),
            jax.ShapeDtypeStruct((3, dp, held, inner), BF16),
        ],
        scratch_shapes=[
            pltpu.VMEM((2 * count, held, sub), BF16),
            pltpu.VMEM((held, inner), F32),
            pltpu.VMEM((held, inner), F32),
            pltpu.VMEM((held, inner), F32),
            pltpu.VMEM((held, inner), BF16),
            pltpu.VMEM((held, inner), BF16),
            pltpu.VMEM((held, inner), BF16),
            pltpu.VMEM((2 * count, held, sub), BF16),
            pltpu.VMEM((2 * count, levels * rows, main), BF16),
            pltpu.VMEM((2 * count, chain, sub + edge), BF16),
            pltpu.VMEM((2 * count, chain, sub + edge), BF16),
            pltpu.VMEM((2 * count, chain, sub + edge), BF16),
            pltpu.VMEM((2 * count, rows, edge), BF16),
            pltpu.VMEM((2 * count, rows, edge), BF16),
            pltpu.VMEM((2 * count, rows, edge), F32),
            pltpu.VMEM((4, sub, half), BF16),
            pltpu.VMEM((2, 2, half, sub), BF16),
            pltpu.VMEM((2, 2, sub, inner), BF16),
            dma((2 * count,)), dma((4,)), dma((2, 2)), dma((2, 2)),
            dma((3,)), dma((2 * count, 3)), dma((3,)), dma((2 * count, 3)),
            dma((levels + 1,)), dma((2 * count, levels)),
            dma((3,)), dma((2 * count, 3)), dma((3,)), dma((2 * count, 3)),
            dma((1,)), dma((2 * count,)),
            dma((levels + 2,)), dma((2, dp, HALVES, levels + 1)),
            dma((3, 3)), dma((3, dp)), dma((3,)),
            dma((1,)), dma((2 * count,)), dma((3,)), dma((2 * count, 3)), dma((2 * count, 3)),
        ],
        compiler_params=pltpu.CompilerParams(
            collective_id=0, has_side_effects=True, vmem_limit_bytes=67_043_328
        ),
        name="fused",
    )(tokens, cotangent, w_gate, w_up, w_down)

    tall = 512 if inner % 512 == 0 else 128
    tile = 256 if part % 256 == 0 else 128
    early, late = inner // tall, part // tile
    depth = dp * held

    def grads(hidden_ref, cot_ref, tok_ref, units_ref, mixed_ref, in_ref, down, gate, up, mixed_out, in_out, both, sem):
        step = pl.program_id(0)

        def fetch(k):
            return pltpu.make_async_copy(units_ref.at[1 + k], both.at[k], sem.at[k])

        def product(left, right):
            return lax.dot_general(
                left.reshape(depth, left.shape[-1]),
                right.reshape(depth, right.shape[-1]),
                (((0,), (0,)), ((), ())),
                preferred_element_type=F32,
            )

        @pl.when(step == 0)
        def _():
            for k in range(2):
                fetch(k).start()
            mixed_out[...] = mixed_ref[...]
            in_out[...] = in_ref[...]

        @pl.when(step < early)
        def _():
            down[...] = product(hidden_ref[...], cot_ref[...])

        @pl.when(step == early)
        def _():
            for k in range(2):
                fetch(k).wait()

        @pl.when(step >= early)
        def _():
            gate[...] = product(tok_ref[...], both[0])
            up[...] = product(tok_ref[...], both[1])

    whole = pl.BlockSpec((rows, width), lambda i: (0, 0))

    def first(i):
        return jnp.minimum(i, early - 1)

    def second(i):
        return jnp.maximum(i - early, 0)

    down_grad, gate_grad, up_grad, mixed, input_grad = pl.pallas_call(
        grads,
        grid=(early + late,),
        in_specs=[
            pl.BlockSpec((None, dp, held, tall), lambda i: (0, 0, 0, first(i))),
            pl.BlockSpec((None, dp, held, part), lambda i: (1, 0, 0, 0)),
            pl.BlockSpec((None, dp, held, tile), lambda i: (0, 0, 0, second(i))),
            hbm,
            whole,
            whole,
        ],
        out_specs=[
            pl.BlockSpec((tall, part), lambda i: (first(i), 0)),
            pl.BlockSpec((tile, inner), lambda i: (second(i), 0)),
            pl.BlockSpec((tile, inner), lambda i: (second(i), 0)),
            whole,
            whole,
        ],
        out_shape=[
            jax.ShapeDtypeStruct((inner, part), F32),
            jax.ShapeDtypeStruct((part, inner), F32),
            jax.ShapeDtypeStruct((part, inner), F32),
            jax.ShapeDtypeStruct((rows, width), BF16),
            jax.ShapeDtypeStruct((rows, width), BF16),
        ],
        scratch_shapes=[pltpu.VMEM((2, dp, held, inner), BF16), dma((2,))],
        compiler_params=pltpu.CompilerParams(vmem_limit_bytes=67_043_328),
        name="grads",
    )(units, features, features, units, mixed, input_grad)
    return mixed, input_grad, gate_grad, up_grad, down_grad


def solution(mesh):
    in_specs = (
        P(("dp", "tp"), None),
        P(None, "tp"),
        P(None, "tp"),
        P("tp", None),
        P(("dp", "tp"), None),
    )
    out_specs = (
        P(("dp", "tp"), None),
        P(("dp", "tp"), None),
        P("dp", "tp"),
        P("dp", "tp"),
        P("tp", "dp"),
    )

    def run(*args):
        chosen = fused_body if (mesh.shape["dp"], mesh.shape["tp"]) == (4, 8) else body
        return chosen(mesh.shape["dp"], mesh.shape["tp"], *args)

    return jax.shard_map(run, mesh=mesh, in_specs=in_specs, out_specs=out_specs, check_vma=False)
```
